32 devices in a mesh: dp: 2 (over y), ep: 16 (over z, x, core).
Axes of the slice: x: 2, y: 2, z: 4, core: 2. Of those that a mesh axis runs over, the one named last changes fastest.
Arguments:
- hidden_in: bfloat16 [768, 4096], P(('dp', 'ep')), may hold values from -6 to 6
- expert_ids: int32 [768, 2], P(('dp', 'ep')), may hold values from 0 to 15, all different within a row; in each aligned block of 24 rows (0 to 23, 24 to 47, ...) at most 4 rows name the same one
- route_logits: float32 [768, 16], P(('dp', 'ep')), may hold values from -10 to 10
- first_weight: bfloat16 [16, 4096, 1024], P('ep', None, 'dp'), may hold values from -0.09375 to 0.09375
- second_weight: bfloat16 [16, 1024, 4096], P('ep', None, 'dp'), may hold values from -0.1875 to 0.1875
- queries: bfloat16 [768, 2048], P(('dp', 'ep')), may hold values from -140 to 140
- span_keys: bfloat16 [768, 2048], P(('dp', 'ep')), may hold values from -7 to 7
- span_values: bfloat16 [768, 2048], P(('dp', 'ep')), may hold values from -6 to 6
- cache_keys: bfloat16 [32, 72, 2048], P(('dp', 'ep')), may hold values from -6 to 6
- cache_values: bfloat16 [32, 72, 2048], P(('dp', 'ep')), may hold values from -6 to 6
- valid_frames: int32 [32], P(('dp', 'ep')), may hold values from 1 to 3
Outputs:
- mixed: bfloat16 [768, 4096], P(('dp', 'ep'))
- attended: bfloat16 [768, 2048], P(('dp', 'ep'))
The draws below stay inside these ranges and needn't reach their ends.
Inputs may be any that keep to these rules, and one draw needn't show every extreme that they name: `expert_ids`: each token names two different experts. In the rows of one device (24 rows) no expert is named more than 4 times, a bound that some block reaches.
All inputs are finite; a program needn't handle non-finite values.
Results may differ from the reference program's by a relative error of at most 0.0057.
Values may be sent and summed in bfloat16 or wider, within the bound.
A program may use at most 128 MiB of HBM per device.

```python
import math
import jax
import jax.numpy as jnp
import numpy as np
from jax import lax

D = 4096
FFN = 1024
HEADS = 16
HEAD_DIM = 128
TOK = 24
FRAME_TOK = 24
CFRAMES = 3
CACHE_TOK = 72
EXPERTS = 16
STREAMS = 32
TOKENS = 768
CAP = 4


def query_key_pair(key):
    width = HEADS * HEAD_DIM
    key_rows = jnp.clip(jax.random.normal(jax.random.fold_in(key, 101), (TOKENS, width), jnp.float32), -6.0, 6.0)
    query_rows = jnp.clip(jax.random.normal(jax.random.fold_in(key, 202), (TOKENS, width), jnp.float32), -6.0, 6.0)
    return (query_rows, key_rows)


def draw_queries(key, part):
    query_rows, key_rows = query_key_pair(key)
    return query_rows.astype(jnp.bfloat16)


def draw_span_keys(key, part):
    query_rows, key_rows = query_key_pair(key)
    return key_rows.astype(jnp.bfloat16)


def set_ends(entries, own_key, low, largest):
    longest = entries.shape.index(max(entries.shape))
    spots = []
    for shift in (0, 1):
        where = [jax.random.randint(jax.random.fold_in(own_key, axis), (), 0, length) for axis, length in enumerate(entries.shape)]
        where[longest] = (where[longest] + shift) % entries.shape[longest]
        spots.append(tuple(where))
    return entries.at[spots[0]].set(low).at[spots[1]].set(largest)


def steps_of(stream_key, dims, pieces, low, high):
    loudness, own = 1.0, jax.random.fold_in(stream_key, 6)
    for dim, shards_of in pieces:
        steps = jnp.exp(jax.random.uniform(jax.random.fold_in(own, dim), (shards_of,), jnp.float32, low / len(pieces), high / len(pieces)))
        loudness = loudness * jnp.repeat(steps, dims[dim] // shards_of).reshape([-1 if axis == dim else 1 for axis in range(len(dims))])
    return loudness


def assign_block(stream_key, own, number, rows, count, top, reach, lean):
    ranking = jax.random.permutation(stream_key, count)
    crowded, ordinary = load_shares(count, rows * top, reach, lean, True), load_shares(count, rows * top, reach, lean, False)
    places = jnp.arange(count)

    def named(lengths, offset_by):
        used = int((lengths > 0).sum())
        fixed = max(1, used // 4)
        passed = fixed + (places - fixed + offset_by * (used - fixed)) % max(1, count - fixed)
        return jnp.zeros((count,), jnp.int32).at[ranking[jnp.where(places < fixed, places, passed)]].set(jnp.asarray(lengths, jnp.int32))

    lengths = jnp.where(number % 4 == 0, named(crowded, number // 4), named(ordinary, number - number // 4 - 1))
    mixed = jax.random.permutation(jax.random.fold_in(own, 3), count)
    giver, receiver = mixed[0:count // 2 * 2:2], mixed[1:count // 2 * 2:2]
    margin = jnp.minimum(lengths[giver] - 1, reach - lengths[receiver]) // 2
    margin = jnp.where((giver == ranking[0]) | (receiver == ranking[0]) | (lengths[receiver] == 0), 0, jnp.maximum(margin, 0))
    passed = jax.random.randint(jax.random.fold_in(own, 4), (count // 2,), 0, 1 << 20) % (margin + 1)
    lengths = lengths.at[giver].add(-passed).at[receiver].add(passed)
    members = jnp.searchsorted(jnp.cumsum(lengths), jnp.arange(rows * top), side="right").astype(jnp.int32)
    listing = members.reshape(top, rows).T
    listing = listing[jax.random.permutation(jax.random.fold_in(own, 1), rows)]
    offset_by = jax.random.randint(jax.random.fold_in(own, 2), (rows, 1), 0, top)
    return jnp.take_along_axis(listing, (jnp.arange(top)[None, :] + offset_by) % top, axis=1)


def load_shares(amount, total, bound, lean, full):
    portions = [(1 << 20) // math.isqrt(rank ** lean) + 1 for rank in range(1, amount + 1)]
    largest = bound if full else min(bound, max(-(-total // amount), total * portions[0] // sum(portions)))
    least = 1 if total - largest >= amount - 1 else 0
    given, surplus = [largest] + [least] * (amount - 1), total - largest - least * (amount - 1)
    while surplus > 0:
        candidates = [i for i in range(1, amount) if given[i] < largest] or [i for i in range(1, amount) if given[i] < bound]
        pool, left = sum([portions[i] for i in candidates]), surplus
        for i in candidates:
            extra = min(bound - given[i], max(1, left * portions[i] // pool), surplus)
            given[i] = given[i] + extra
            surplus = surplus - extra
    return np.array(given)


def centred(key, extent, deviation, limit, pieces=(), kind=jnp.bfloat16):
    array = deviation * jax.random.normal(key, extent, jnp.float32)
    if pieces:
        array = array * steps_of(key, extent, pieces, -0.22, 0.18)
    return jnp.clip(array, -limit, limit).astype(kind)


def setup_inputs(seed: int = 0) -> dict:
    key_list = jax.random.split(jax.random.key(seed), 12)
    hidden_in = centred(key_list[0], (TOKENS, D), 1.0, 6.0, ((0, 32),))
    expert_ids_keys = jax.random.split(jax.random.fold_in(key_list[1], 1), TOKENS // TOK)
    expert_ids_turns = jax.random.permutation(jax.random.fold_in(key_list[1], 3), TOKENS // TOK)
    expert_ids = jax.vmap(lambda own, number: assign_block(jax.random.fold_in(key_list[1], 2), own, number, TOK, EXPERTS, 2, CAP, 2))(expert_ids_keys, expert_ids_turns).reshape((TOKENS, 2))
    route_logits = centred(key_list[2], (TOKENS, EXPERTS), 2.0, 10.0, ((0, 32),), jnp.float32)
    first_weight = centred(key_list[3], (EXPERTS, D, FFN), D ** -0.5, 0.09375, ((0, 16), (2, 2)))
    second_weight = centred(key_list[4], (EXPERTS, FFN, D), FFN ** -0.5, 0.1875, ((0, 16), (2, 2)))
    queries = draw_queries(jax.random.fold_in(key_list[11], 71), 0)
    span_keys = draw_span_keys(jax.random.fold_in(key_list[11], 71), 0)
    span_values = centred(key_list[7], (TOKENS, HEADS * HEAD_DIM), 1.0, 6.0, ((0, 32),))
    cache_keys = centred(key_list[8], (STREAMS, CACHE_TOK, HEADS * HEAD_DIM), 1.0, 6.0, ((0, 32),))
    cache_values = centred(key_list[9], (STREAMS, CACHE_TOK, HEADS * HEAD_DIM), 1.0, 6.0, ((0, 32),))
    valid_frames = set_ends(jax.random.randint(key_list[10], (STREAMS,), 1, CFRAMES + 1), jax.random.fold_in(key_list[10], 1), 1, CFRAMES).astype(jnp.int32)
    return dict(hidden_in=hidden_in, expert_ids=expert_ids, route_logits=route_logits, first_weight=first_weight, second_weight=second_weight, queries=queries, span_keys=span_keys, span_values=span_values, cache_keys=cache_keys, cache_values=cache_values, valid_frames=valid_frames)


def activate(pre):
    return jax.nn.gelu(pre, approximate=True).astype(jnp.bfloat16)

def attend(queries, span_keys, span_values, cache_keys, cache_values, valid_count):
    token_count = queries.shape[0]
    cache_len = cache_keys.shape[0]
    key_rows = jnp.concatenate([cache_keys, span_keys], axis=0)
    value_rows = jnp.concatenate([cache_values, span_values], axis=0)
    query_heads = queries.reshape(token_count, HEADS, HEAD_DIM).astype(jnp.float32)
    key_heads = key_rows.reshape(-1, HEADS, HEAD_DIM).astype(jnp.float32)
    value_heads = value_rows.reshape(-1, HEADS, HEAD_DIM).astype(jnp.float32)
    scores = jnp.einsum('thd,khd->htk', query_heads, key_heads) * (1.0 / math.sqrt(HEAD_DIM))
    position = jnp.arange(key_rows.shape[0], dtype=jnp.int32)
    usable = (position >= cache_len) | (position // FRAME_TOK < valid_count)
    scores = jnp.where(usable[None, None, :], scores, -1e+30)
    row_max = lax.optimization_barrier(jnp.max(scores, axis=2, keepdims=True))
    weights = jnp.exp(scores - row_max)
    weights = (weights / lax.optimization_barrier(jnp.sum(weights, axis=2, keepdims=True))).astype(jnp.bfloat16)
    result = jnp.einsum('htk,khd->thd', weights.astype(jnp.float32), value_heads)
    return result.astype(jnp.bfloat16).reshape(token_count, HEADS * HEAD_DIM)

def block_slots(expert_ids):
    assigned = TOK * 2
    blocks = expert_ids.reshape(STREAMS, assigned)
    row_ids = lax.broadcasted_iota(jnp.int32, (assigned, assigned), 0)
    col_ids = lax.broadcasted_iota(jnp.int32, (assigned, assigned), 1)

    def per_block(flat_ids):
        same_expert = (flat_ids[:, None] == flat_ids[None, :]) & (col_ids < row_ids)
        return lax.optimization_barrier(jnp.sum(same_expert.astype(jnp.int32), axis=1))
    return jax.vmap(per_block)(blocks).reshape(TOKENS, 2)

def reference(hidden_in, expert_ids, route_logits, first_weight, second_weight, queries, span_keys, span_values, cache_keys, cache_values, valid_frames):
    slots = block_slots(expert_ids)
    token_index = jnp.arange(TOKENS, dtype=jnp.int32)
    stream_of = token_index // TOK
    rows_at = (stream_of[:, None] * CAP + slots).astype(jnp.int32)
    slot_table = jnp.full((EXPERTS, STREAMS * CAP), TOKENS, jnp.int32)
    slot_table = slot_table.at[expert_ids, rows_at].set(jnp.broadcast_to(token_index[:, None], (TOKENS, 2)))
    padded = jnp.concatenate([hidden_in, jnp.zeros((1, D), jnp.bfloat16)], axis=0)

    def apply_expert(operands):
        first_matrix, second_matrix, index_row = operands
        expert_rows = padded[index_row]
        hidden = activate(jnp.dot(expert_rows, first_matrix, preferred_element_type=jnp.float32))
        return jnp.dot(hidden, second_matrix, preferred_element_type=jnp.float32).astype(jnp.bfloat16)
    expert_outs = lax.map(apply_expert, (first_weight, second_weight, slot_table))
    chosen = jnp.take_along_axis(route_logits, expert_ids, axis=1)
    gates = jax.nn.softmax(chosen, axis=1)
    running = jnp.zeros((TOKENS, D), jnp.float32)
    for column in range(2):
        picked = expert_outs[expert_ids[:, column], rows_at[:, column]].astype(jnp.float32)
        running = running + gates[:, column:column + 1] * picked
    mixed = running.astype(jnp.bfloat16)
    width = HEADS * HEAD_DIM
    attended = jax.vmap(attend)(queries.reshape(STREAMS, TOK, width), span_keys.reshape(STREAMS, TOK, width), span_values.reshape(STREAMS, TOK, width), cache_keys, cache_values, valid_frames).reshape(TOKENS, width)
    return (mixed, attended)
```

```python
import functools
import math

import jax
import jax.numpy as jnp
from jax import lax
from jax.experimental import pallas as pl
from jax.experimental.pallas import tpu as pltpu
from jax.sharding import PartitionSpec as P

HEAD_DIM = 128
FRAME_TOK = 24
TILE = 16
MESH = pl.DeviceIdType.MESH


def iota(shape, axis):
    return lax.broadcasted_iota(jnp.int32, shape, axis)


def as_bf16(mask):
    return jnp.where(mask, 1.0, 0.0).astype(jnp.bfloat16)


def log2(n):
    return n.bit_length() - 1


def flip(me, off, n):
    out = jnp.int32(0)
    bit = 1
    while bit < n:
        one = jnp.int32(bit)
        out = out + one * lax.rem(lax.div(me, one) + lax.div(off, one), jnp.int32(2))
        bit *= 2
    return out


def fold_map(shape, long_axis, group, cap):
    long, tiled = iota(shape, long_axis), iota(shape, 1 - long_axis)
    fold = long >> log2(group * cap)
    source = (long & (group * cap - 1)) >> log2(cap)
    slot = long & (cap - 1)
    return as_bf16(tiled == source * TILE + fold * cap + slot)


def dot(a, b):
    return jnp.dot(a, b, preferred_element_type=jnp.float32)


def drain(view, sem):
    pltpu.make_async_copy(view, view, sem).wait()


def attend(q, k, v, ck, cv, frames, out):
    cache_len = ck.shape[0]
    scale = 1.0 / math.sqrt(HEAD_DIM)
    usable = (iota((1, cache_len), 1) // FRAME_TOK) < frames
    contract = (((1,), (1,)), ((), ()))
    for head in range(q.shape[1] // HEAD_DIM):
        cols = slice(head * HEAD_DIM, (head + 1) * HEAD_DIM)
        query = q[:, cols]
        old = lax.dot_general(query, ck[:, cols], contract, preferred_element_type=jnp.float32)
        new = lax.dot_general(query, k[:, cols], contract, preferred_element_type=jnp.float32)
        old = jnp.where(usable, old * scale, -1e30)
        new = new * scale
        top = jnp.maximum(
            jnp.max(old, axis=1, keepdims=True), jnp.max(new, axis=1, keepdims=True)
        )
        old = jnp.exp(old - top)
        new = jnp.exp(new - top)
        total = jnp.sum(old, axis=1, keepdims=True) + jnp.sum(new, axis=1, keepdims=True)
        old = (old / total).astype(jnp.bfloat16)
        new = (new / total).astype(jnp.bfloat16)
        out[:, cols] = (dot(old, cv[:, cols]) + dot(new, v[:, cols])).astype(jnp.bfloat16)


def kernel(
    dp_n, ep_n, cap, back_folds,
    ids, logits, frames, hidden,
    q_hbm, k_hbm, v_hbm, ck_hbm, cv_hbm, w1_hbm, w2_hbm,
    mixed, attended,
    w1, w2, q, k, v, ck, cv,
    disp, rows, xs, hid, ys, back_out, back_in,
    load_sem, disp_send, disp_recv, relay_send, relay_recv,
    hid_send, hid_recv, back_send, back_recv, own_sem,
):
    d, me = lax.axis_index("dp"), lax.axis_index("ep")
    tokens = hidden.shape[0]
    folds = TILE // cap
    fold_cols = disp.shape[2]
    back_cols = back_in.shape[2]
    group = min(ep_n, 16)
    group_rows = group * cap
    total = dp_n * ep_n

    barrier = pltpu.get_barrier_semaphore()

    def greet(i, carry):
        other = lax.rem(d * ep_n + me + i, jnp.int32(total))
        pl.semaphore_signal(
            barrier,
            inc=1,
            device_id={
                "dp": lax.div(other, jnp.int32(ep_n)),
                "ep": lax.rem(other, jnp.int32(ep_n)),
            },
            device_id_type=MESH,
        )
        return carry

    lax.fori_loop(1, total, greet, 0)

    loads = [
        pltpu.make_async_copy(src, dst, load_sem.at[i])
        for i, (src, dst) in enumerate(
            [(w1_hbm, w1), (w2_hbm, w2), (q_hbm, q), (k_hbm, k), (v_hbm, v), (ck_hbm, ck), (cv_hbm, cv)]
        )
    ]
    for load in loads:
        load.start()

    experts = iota((tokens, ep_n), 1)
    named = [experts == ids[:, c : c + 1] for c in range(2)]
    count = as_bf16(named[0] | named[1])
    earlier = as_bf16(iota((tokens, tokens), 1) < iota((tokens, tokens), 0))
    before = dot(earlier, count)
    place, place_row, chosen = [], [], []
    eye = iota((tokens, tokens), 0) == iota((tokens, tokens), 1)
    for c in range(2):
        slot = jnp.sum(jnp.where(named[c], before, 0.0), axis=1, keepdims=True).astype(jnp.int32)
        place.append(ids[:, c : c + 1] * TILE + slot)
        place_row.append(jnp.sum(jnp.where(eye, place[c], 0), axis=0, keepdims=True))
        chosen.append(jnp.sum(jnp.where(named[c], logits[...], 0.0), axis=1, keepdims=True))
    top = jnp.maximum(chosen[0], chosen[1])
    powers = [jnp.exp(x - top) for x in chosen]
    gates = [p / (powers[0] + powers[1]) for p in powers]

    row_at = iota((ep_n * TILE, tokens), 0)
    pickers = [
        as_bf16((row_at - f * cap == place_row[0]) | (row_at - f * cap == place_row[1]))
        for f in range(folds)
    ]
    step = min(fold_cols, 256)
    for at in range(0, fold_cols, step):
        acc = dot(pickers[0], hidden[:, at : at + step])
        for f in range(1, folds):
            acc += dot(pickers[f], hidden[:, f * fold_cols + at : f * fold_cols + at + step])
        disp[:, :, at : at + step] = acc.astype(jnp.bfloat16).reshape(ep_n, TILE, step)

    pl.semaphore_wait(barrier, total - 1)

    def dispatch(i, carry):
        target = flip(me, ep_n - 1 - i, ep_n)
        pltpu.make_async_remote_copy(
            src_ref=disp.at[target],
            dst_ref=rows.at[d * ep_n + me],
            send_sem=disp_send,
            recv_sem=disp_recv.at[me],
            device_id={"dp": d, "ep": target},
            device_id_type=MESH,
        ).start()
        return carry

    lax.fori_loop(0, ep_n - 1, dispatch, 0)
    pltpu.make_async_copy(disp.at[me], rows.at[d * ep_n + me], disp_recv.at[me]).start()

    def relay(off):
        source = flip(me, off, ep_n)
        chunk = rows.at[d * ep_n + source]
        drain(chunk, disp_recv.at[source])
        for j in range(1, dp_n):
            pltpu.make_async_remote_copy(
                src_ref=chunk,
                dst_ref=chunk,
                send_sem=relay_send,
                recv_sem=relay_recv.at[d],
                device_id={"dp": lax.rem(d + j, jnp.int32(dp_n)), "ep": me},
                device_id_type=MESH,
            ).start()

    near = min(4, ep_n)

    def relay_near(i, carry):
        relay(i)
        return carry

    def relay_far(i, carry):
        relay(ep_n - 1 + near - i)
        return carry

    lax.fori_loop(0, near, relay_near, 0)
    lax.fori_loop(near, ep_n, relay_far, 0)

    unfold = fold_map((folds * group_rows, group * TILE), 0, group, cap)
    refold = fold_map((group * TILE, back_folds * group_rows), 1, group, cap)

    loads[0].wait()
    loads[1].wait()
    for j in range(dp_n):
        plane = lax.rem(d + j, jnp.int32(dp_n))
        if j > 0:
            drain(rows.at[pl.ds(plane * ep_n, ep_n)], relay_recv.at[plane])
        for g in range(ep_n // group):
            tiles = rows[pl.ds(plane * ep_n + g * group, group)].reshape(group * TILE, fold_cols)
            flat = dot(unfold, tiles).astype(jnp.bfloat16)
            for f in range(folds):
                xs[f, g * group_rows : (g + 1) * group_rows, :] = flat[
                    f * group_rows : (f + 1) * group_rows
                ]
        acc = dot(xs[0], w1[:fold_cols, :])
        for f in range(1, folds):
            acc += dot(xs[f], w1[f * fold_cols : (f + 1) * fold_cols, :])
        hid[plane * dp_n + d] = jax.nn.gelu(acc, approximate=True).astype(jnp.bfloat16)
        for i in range(1, dp_n):
            pltpu.make_async_remote_copy(
                src_ref=hid.at[plane * dp_n + d],
                dst_ref=hid.at[plane * dp_n + d],
                send_sem=hid_send,
                recv_sem=hid_recv.at[plane * dp_n + d],
                device_id={"dp": lax.rem(d + i, jnp.int32(dp_n)), "ep": me},
                device_id_type=MESH,
            ).start()

    units = hid.shape[2]
    for j in range(dp_n):
        plane = lax.rem(d + j, jnp.int32(dp_n))
        for i in range(1, dp_n):
            part = plane * dp_n + lax.rem(d + i, jnp.int32(dp_n))
            drain(hid.at[part], hid_recv.at[part])
        for f in range(back_folds):
            cols = slice(f * back_cols, (f + 1) * back_cols)
            acc = dot(hid[plane * dp_n], w2[:units, cols])
            for i in range(1, dp_n):
                acc += dot(hid[plane * dp_n + i], w2[i * units : (i + 1) * units, cols])
            ys[f] = acc.astype(jnp.bfloat16)
        for g in range(ep_n // group):
            flat = jnp.concatenate(
                [ys[f, g * group_rows : (g + 1) * group_rows, :] for f in range(back_folds)], axis=0
            )
            tiles = dot(refold, flat).astype(jnp.bfloat16)
            back_out[pl.ds(plane * ep_n + g * group, group)] = tiles.reshape(group, TILE, back_cols)

        def give_back(i, carry):
            target = flip(me, ep_n - 1 - i, ep_n)
            pltpu.make_async_remote_copy(
                src_ref=back_out.at[plane * ep_n + target],
                dst_ref=back_in.at[d * ep_n + me],
                send_sem=back_send,
                recv_sem=back_recv,
                device_id={"dp": plane, "ep": target},
                device_id_type=MESH,
            ).start()
            return carry

        lax.fori_loop(0, ep_n - 1 if j == 0 else ep_n, give_back, 0)
        if j == 0:
            pltpu.make_async_copy(
                back_out.at[d * ep_n + me], back_in.at[d * ep_n + me], own_sem
            ).start()

    for load in loads[2:]:
        load.wait()
    attend(q, k, v, ck, cv, frames[0], attended)

    col_at = iota((tokens, ep_n * TILE), 1)
    picks = jnp.concatenate(
        [
            jnp.where(col_at - f * cap == place[c], 1.0, 0.0)
            for f in range(back_folds)
            for c in range(2)
        ],
        axis=0,
    ).astype(jnp.bfloat16)

    drain(back_in.at[pl.ds(0, total - 1)], back_recv)
    drain(back_in.at[0], own_sem)
    for h in range(dp_n):
        tiles = back_in[h * ep_n : (h + 1) * ep_n].reshape(ep_n * TILE, back_cols)
        picked = dot(picks, tiles)
        for f in range(back_folds):
            at = 2 * f * tokens
            cols = slice((h * back_folds + f) * back_cols, (h * back_folds + f + 1) * back_cols)
            mixed[:, cols] = (
                gates[0] * picked[at : at + tokens] + gates[1] * picked[at + tokens : at + 2 * tokens]
            ).astype(jnp.bfloat16)

    drain(disp.at[pl.ds(0, ep_n - 1)], disp_send)
    if dp_n > 1:
        drain(rows.at[pl.ds(0, (dp_n - 1) * ep_n)], relay_send)
        drain(hid.at[pl.ds(0, dp_n * (dp_n - 1))], hid_send)
    drain(back_out.at[pl.ds(0, total - 1)], back_send)


def shards(dp_n, ep_n, *args):
    (hidden_in, expert_ids, route_logits, first_weight, second_weight,
     queries, span_keys, span_values, cache_keys, cache_values, valid_frames) = args
    tokens, width = hidden_in.shape
    cap = max(2, 8 * tokens // (3 * ep_n))
    _, _, units = first_weight.shape
    _, all_units, cols = second_weight.shape
    folds = TILE // cap
    back_folds = min(folds, cols // 128)
    slots = ep_n * cap
    bf16 = jnp.bfloat16
    vmem, hbm = pl.BlockSpec(memory_space=pltpu.VMEM), pl.BlockSpec(memory_space=pl.ANY)
    dma = pltpu.SemaphoreType.DMA
    total = dp_n * ep_n
    return pl.pallas_call(
        functools.partial(kernel, dp_n, ep_n, cap, back_folds),
        out_shape=(
            jax.ShapeDtypeStruct((tokens, width), bf16),
            jax.ShapeDtypeStruct(queries.shape, bf16),
        ),
        in_specs=[vmem, vmem, pl.BlockSpec(memory_space=pltpu.SMEM), vmem] + [hbm] * 7,
        out_specs=(vmem, vmem),
        scratch_shapes=[
            pltpu.VMEM((width, units), bf16),
            pltpu.VMEM((all_units, cols), bf16),
            pltpu.VMEM(queries.shape, bf16),
            pltpu.VMEM(span_keys.shape, bf16),
            pltpu.VMEM(span_values.shape, bf16),
            pltpu.VMEM(cache_keys.shape[1:], bf16),
            pltpu.VMEM(cache_values.shape[1:], bf16),
            pltpu.VMEM((ep_n, TILE, width // folds), bf16),
            pltpu.VMEM((total, TILE, width // folds), bf16),
            pltpu.VMEM((folds, slots, width // folds), bf16),
            pltpu.VMEM((dp_n * dp_n, slots, units), bf16),
            pltpu.VMEM((back_folds, slots, cols // back_folds), bf16),
            pltpu.VMEM((total, TILE, cols // back_folds), bf16),
            pltpu.VMEM((total, TILE, cols // back_folds), bf16),
            dma((7,)),
            dma(()),
            dma((ep_n,)),
            dma(()),
            dma((dp_n,)),
            dma(()),
            dma((dp_n * dp_n,)),
            dma(()),
            dma(()),
            dma(()),
        ],
        compiler_params=pltpu.CompilerParams(
            collective_id=0, has_side_effects=True, vmem_limit_bytes=60 * 1024 * 1024
        ),
    )(
        expert_ids, route_logits, valid_frames, hidden_in,
        queries, span_keys, span_values, cache_keys[0], cache_values[0],
        first_weight[0], second_weight[0],
    )


def solution(mesh):
    tokens = P(("dp", "ep"), None)
    weights = P("ep", None, "dp")
    cache = P(("dp", "ep"), None, None)
    return jax.shard_map(
        functools.partial(shards, mesh.shape["dp"], mesh.shape["ep"]),
        mesh=mesh,
        in_specs=(
            tokens, tokens, tokens, weights, weights, tokens, tokens, tokens, cache, cache,
            P(("dp", "ep")),
        ),
        out_specs=(tokens, tokens),
        check_vma=False,
    )
```

```python
import functools
import math

import jax
import jax.numpy as jnp
from jax import lax
from jax.experimental import pallas as pl
from jax.experimental.pallas import tpu as pltpu
from jax.sharding import PartitionSpec as P

HEAD_DIM = 128
FRAME_TOK = 24
TILE = 16
MESH = pl.DeviceIdType.MESH


def iota(shape, axis):
    return lax.broadcasted_iota(jnp.int32, shape, axis)


def as_bf16(mask):
    return jnp.where(mask, 1.0, 0.0).astype(jnp.bfloat16)


def log2(n):
    return n.bit_length() - 1


def flip(me, off, n):
    out = jnp.int32(0)
    bit = 1
    while bit < n:
        one = jnp.int32(bit)
        out = out + one * lax.rem(lax.div(me, one) + lax.div(off, one), jnp.int32(2))
        bit *= 2
    return out


def fold_map(shape, long_axis, group, cap):
    long, tiled = iota(shape, long_axis), iota(shape, 1 - long_axis)
    fold = long >> log2(group * cap)
    source = (long & (group * cap - 1)) >> log2(cap)
    slot = long & (cap - 1)
    return as_bf16(tiled == source * TILE + fold * cap + slot)


def dot(a, b):
    return jnp.dot(a, b, preferred_element_type=jnp.float32)


def drain(view, sem):
    pltpu.make_async_copy(view, view, sem).wait()


def attend(q, k, v, ck, cv, frames, out):
    cache_len = ck.shape[0]
    scale = 1.0 / math.sqrt(HEAD_DIM)
    usable = (iota((1, cache_len), 1) // FRAME_TOK) < frames
    contract = (((1,), (1,)), ((), ()))
    for head in range(q.shape[1] // HEAD_DIM):
        cols = slice(head * HEAD_DIM, (head + 1) * HEAD_DIM)
        query = q[:, cols]
        old = lax.dot_general(query, ck[:, cols], contract, preferred_element_type=jnp.float32)
        new = lax.dot_general(query, k[:, cols], contract, preferred_element_type=jnp.float32)
        old = jnp.where(usable, old * scale, -1e30)
        new = new * scale
        top = jnp.maximum(
            jnp.max(old, axis=1, keepdims=True), jnp.max(new, axis=1, keepdims=True)
        )
        old = jnp.exp(old - top)
        new = jnp.exp(new - top)
        total = jnp.sum(old, axis=1, keepdims=True) + jnp.sum(new, axis=1, keepdims=True)
        old = (old / total).astype(jnp.bfloat16)
        new = (new / total).astype(jnp.bfloat16)
        out[:, cols] = (dot(old, cv[:, cols]) + dot(new, v[:, cols])).astype(jnp.bfloat16)


def kernel(
    dp_n, ep_n, cap, back_folds,
    frames, ids_hbm, logits_hbm, hidden_hbm,
    q_hbm, k_hbm, v_hbm, ck_hbm, cv_hbm, w1_hbm, w2_hbm,
    mixed, attended,
    ids, logits, hidden, w1, w2, q, k, v, ck, cv,
    disp, rows, xs, hid, ys, back_out, back_in,
    load_sem, disp_send, disp_recv, relay_send, relay_recv,
    hid_send, hid_recv, back_send, back_recv, own_sem,
):
    d, me = lax.axis_index("dp"), lax.axis_index("ep")
    tokens = hidden.shape[0]
    folds = TILE // cap
    fold_cols = disp.shape[2]
    back_cols = back_in.shape[2]
    group = min(ep_n, 16)
    group_rows = group * cap
    total = dp_n * ep_n

    barrier = pltpu.get_barrier_semaphore()

    def greet(i, carry):
        pl.semaphore_signal(
            barrier, inc=1, device_id={"dp": d, "ep": flip(me, i, ep_n)}, device_id_type=MESH
        )
        return carry

    lax.fori_loop(1, ep_n, greet, 0)
    for i in range(1, dp_n):
        pl.semaphore_signal(
            barrier,
            inc=1,
            device_id={"dp": lax.rem(d + i, jnp.int32(dp_n)), "ep": me},
            device_id_type=MESH,
        )

    loads = [
        pltpu.make_async_copy(src, dst, load_sem.at[i])
        for i, (src, dst) in enumerate(
            [
                (ids_hbm, ids), (logits_hbm, logits), (hidden_hbm, hidden),
                (w1_hbm, w1), (w2_hbm, w2),
                (q_hbm, q), (k_hbm, k), (v_hbm, v), (ck_hbm, ck), (cv_hbm, cv),
            ]
        )
    ]
    for load in loads:
        load.start()
    for load in loads[:3]:
        load.wait()

    experts = iota((ep_n, tokens), 0)
    named = [experts == ids[c : c + 1, :] for c in range(2)]
    count = as_bf16(named[0] | named[1])
    earlier = as_bf16(iota((tokens, tokens), 0) < iota((tokens, tokens), 1))
    before = dot(count, earlier)
    eye = iota((tokens, tokens), 0) == iota((tokens, tokens), 1)
    place, place_row, chosen = [], [], []
    for c in range(2):
        slot = jnp.sum(jnp.where(named[c], before, 0.0), axis=0, keepdims=True).astype(jnp.int32)
        place_row.append(ids[c : c + 1, :] * TILE + slot)
        place.append(jnp.sum(jnp.where(eye, place_row[c], 0), axis=1, keepdims=True))
        chosen.append(jnp.sum(jnp.where(named[c], logits[...], 0.0), axis=0, keepdims=True))
    top = jnp.maximum(chosen[0], chosen[1])
    powers = [jnp.exp(x - top) for x in chosen]
    gates = [
        jnp.sum(jnp.where(eye, p / (powers[0] + powers[1]), 0.0), axis=1, keepdims=True)
        for p in powers
    ]

    row_at = iota((ep_n * TILE, tokens), 0)
    pickers = [
        as_bf16((row_at - f * cap == place_row[0]) | (row_at - f * cap == place_row[1]))
        for f in range(folds)
    ]
    step = min(fold_cols, 256)
    for at in range(0, fold_cols, step):
        acc = dot(pickers[0], hidden[:, at : at + step])
        for f in range(1, folds):
            acc += dot(pickers[f], hidden[:, f * fold_cols + at : f * fold_cols + at + step])
        disp[:, :, at : at + step] = acc.astype(jnp.bfloat16).reshape(ep_n, TILE, step)

    pl.semaphore_wait(barrier, ep_n + dp_n - 2)

    def dispatch(off, carry):
        target = flip(me, off, ep_n)
        pltpu.make_async_remote_copy(
            src_ref=disp.at[target],
            dst_ref=rows.at[d * ep_n + me],
            send_sem=disp_send,
            recv_sem=disp_recv.at[me],
            device_id={"dp": d, "ep": target},
            device_id_type=MESH,
        ).start()
        return carry

    lax.fori_loop(1, ep_n, dispatch, 0)
    pltpu.make_async_copy(disp.at[me], rows.at[d * ep_n + me], disp_recv.at[me]).start()

    def relay(off, carry):
        source = flip(me, off, ep_n)
        chunk = rows.at[d * ep_n + source]
        drain(chunk, disp_recv.at[source])
        for j in range(1, dp_n):
            pltpu.make_async_remote_copy(
                src_ref=chunk,
                dst_ref=chunk,
                send_sem=relay_send,
                recv_sem=relay_recv.at[d],
                device_id={"dp": lax.rem(d + j, jnp.int32(dp_n)), "ep": me},
                device_id_type=MESH,
            ).start()
        return carry

    lax.fori_loop(0, ep_n, relay, 0)

    unfold = fold_map((folds * group_rows, group * TILE), 0, group, cap)
    refold = fold_map((group * TILE, back_folds * group_rows), 1, group, cap)

    loads[3].wait()
    loads[4].wait()
    for j in range(dp_n):
        plane = lax.rem(d + j, jnp.int32(dp_n))
        if j > 0:
            drain(rows.at[pl.ds(plane * ep_n, ep_n)], relay_recv.at[plane])
        for g in range(ep_n // group):
            tiles = rows[pl.ds(plane * ep_n + g * group, group)].reshape(group * TILE, fold_cols)
            flat = dot(unfold, tiles).astype(jnp.bfloat16)
            for f in range(folds):
                xs[f, g * group_rows : (g + 1) * group_rows, :] = flat[
                    f * group_rows : (f + 1) * group_rows
                ]
        acc = dot(xs[0], w1[:fold_cols, :])
        for f in range(1, folds):
            acc += dot(xs[f], w1[f * fold_cols : (f + 1) * fold_cols, :])
        hid[plane * dp_n + d] = jax.nn.gelu(acc, approximate=True).astype(jnp.bfloat16)
        for i in range(1, dp_n):
            pltpu.make_async_remote_copy(
                src_ref=hid.at[plane * dp_n + d],
                dst_ref=hid.at[plane * dp_n + d],
                send_sem=hid_send,
                recv_sem=hid_recv.at[plane * dp_n + d],
                device_id={"dp": lax.rem(d + i, jnp.int32(dp_n)), "ep": me},
                device_id_type=MESH,
            ).start()

    units = hid.shape[2]
    for j in range(dp_n):
        plane = lax.rem(d + j, jnp.int32(dp_n))
        for i in range(1, dp_n):
            part = plane * dp_n + lax.rem(d + i, jnp.int32(dp_n))
            drain(hid.at[part], hid_recv.at[part])
        for f in range(back_folds):
            cols = slice(f * back_cols, (f + 1) * back_cols)
            acc = dot(hid[plane * dp_n], w2[:units, cols])
            for i in range(1, dp_n):
                acc += dot(hid[plane * dp_n + i], w2[i * units : (i + 1) * units, cols])
            ys[f] = acc.astype(jnp.bfloat16)
        for g in range(ep_n // group):
            flat = jnp.concatenate(
                [ys[f, g * group_rows : (g + 1) * group_rows, :] for f in range(back_folds)], axis=0
            )
            tiles = dot(refold, flat).astype(jnp.bfloat16)
            back_out[pl.ds(plane * ep_n + g * group, group)] = tiles.reshape(group, TILE, back_cols)

        def give_back(off, carry):
            target = flip(me, off, ep_n)
            pltpu.make_async_remote_copy(
                src_ref=back_out.at[plane * ep_n + target],
                dst_ref=back_in.at[d * ep_n + me],
                send_sem=back_send,
                recv_sem=back_recv,
                device_id={"dp": plane, "ep": target},
                device_id_type=MESH,
            ).start()
            return carry

        lax.fori_loop(1 if j == 0 else 0, ep_n, give_back, 0)
        if j == 0:
            pltpu.make_async_copy(
                back_out.at[d * ep_n + me], back_in.at[d * ep_n + me], own_sem
            ).start()

    for load in loads[5:]:
        load.wait()
    attend(q, k, v, ck, cv, frames[0], attended)

    col_at = iota((tokens, ep_n * TILE), 1)
    picks = jnp.concatenate(
        [
            jnp.where(col_at - f * cap == place[c], 1.0, 0.0)
            for f in range(back_folds)
            for c in range(2)
        ],
        axis=0,
    ).astype(jnp.bfloat16)

    drain(back_in.at[pl.ds(0, total - 1)], back_recv)
    drain(back_in.at[0], own_sem)
    for h in range(dp_n):
        tiles = back_in[h * ep_n : (h + 1) * ep_n].reshape(ep_n * TILE, back_cols)
        picked = dot(picks, tiles)
        for f in range(back_folds):
            at = 2 * f * tokens
            cols = slice((h * back_folds + f) * back_cols, (h * back_folds + f + 1) * back_cols)
            mixed[:, cols] = (
                gates[0] * picked[at : at + tokens] + gates[1] * picked[at + tokens : at + 2 * tokens]
            ).astype(jnp.bfloat16)

    drain(disp.at[pl.ds(0, ep_n - 1)], disp_send)
    if dp_n > 1:
        drain(rows.at[pl.ds(0, (dp_n - 1) * ep_n)], relay_send)
        drain(hid.at[pl.ds(0, dp_n * (dp_n - 1))], hid_send)
    drain(back_out.at[pl.ds(0, total - 1)], back_send)


def shards(dp_n, ep_n, *args):
    (hidden_in, expert_ids, route_logits, first_weight, second_weight,
     queries, span_keys, span_values, cache_keys, cache_values, valid_frames) = args
    tokens, width = hidden_in.shape
    cap = max(2, 8 * tokens // (3 * ep_n))
    _, _, units = first_weight.shape
    _, all_units, cols = second_weight.shape
    folds = TILE // cap
    back_folds = min(folds, cols // 128)
    slots = ep_n * cap
    bf16 = jnp.bfloat16
    vmem, hbm = pl.BlockSpec(memory_space=pltpu.VMEM), pl.BlockSpec(memory_space=pltpu.HBM)
    dma = pltpu.SemaphoreType.DMA
    total = dp_n * ep_n
    streamed = (
        expert_ids.T, route_logits.T, hidden_in,
        queries, span_keys, span_values, cache_keys[0], cache_values[0],
        first_weight[0], second_weight[0],
    )
    return pl.pallas_call(
        functools.partial(kernel, dp_n, ep_n, cap, back_folds),
        out_shape=(
            jax.ShapeDtypeStruct((tokens, width), bf16),
            jax.ShapeDtypeStruct(queries.shape, bf16),
        ),
        in_specs=[pl.BlockSpec(memory_space=pltpu.SMEM)] + [hbm] * len(streamed),
        out_specs=(vmem, vmem),
        scratch_shapes=[
            pltpu.VMEM((2, tokens), jnp.int32),
            pltpu.VMEM((ep_n, tokens), jnp.float32),
            pltpu.VMEM((tokens, width), bf16),
            pltpu.VMEM((width, units), bf16),
            pltpu.VMEM((all_units, cols), bf16),
            pltpu.VMEM(queries.shape, bf16),
            pltpu.VMEM(span_keys.shape, bf16),
            pltpu.VMEM(span_values.shape, bf16),
            pltpu.VMEM(cache_keys.shape[1:], bf16),
            pltpu.VMEM(cache_values.shape[1:], bf16),
            pltpu.VMEM((ep_n, TILE, width // folds), bf16),
            pltpu.VMEM((total, TILE, width // folds), bf16),
            pltpu.VMEM((folds, slots, width // folds), bf16),
            pltpu.VMEM((dp_n * dp_n, slots, units), bf16),
            pltpu.VMEM((back_folds, slots, cols // back_folds), bf16),
            pltpu.VMEM((total, TILE, cols // back_folds), bf16),
            pltpu.VMEM((total, TILE, cols // back_folds), bf16),
            dma((len(streamed),)),
            dma(()),
            dma((ep_n,)),
            dma(()),
            dma((dp_n,)),
            dma(()),
            dma((dp_n * dp_n,)),
            dma(()),
            dma(()),
            dma(()),
        ],
        compiler_params=pltpu.CompilerParams(
            collective_id=0, has_side_effects=True, vmem_limit_bytes=40 * 1024 * 1024
        ),
    )(
        valid_frames,
        *[pltpu.with_memory_space_constraint(x, pltpu.HBM) for x in streamed],
    )


def solution(mesh):
    tokens = P(("dp", "ep"), None)
    weights = P("ep", None, "dp")
    cache = P(("dp", "ep"), None, None)
    return jax.shard_map(
        functools.partial(shards, mesh.shape["dp"], mesh.shape["ep"]),
        mesh=mesh,
        in_specs=(
            tokens, tokens, tokens, weights, weights, tokens, tokens, tokens, cache, cache,
            P(("dp", "ep")),
        ),
        out_specs=(tokens, tokens),
        check_vma=False,
    )
```

```python
import functools
import math

import jax
import jax.numpy as jnp
from jax import lax
from jax.experimental import pallas as pl
from jax.experimental.pallas import tpu as pltpu
from jax.sharding import PartitionSpec as P

HEAD_DIM = 128
FRAME_TOK = 24
TILE = 16
MESH = pl.DeviceIdType.MESH


def iota(shape, axis):
    return lax.broadcasted_iota(jnp.int32, shape, axis)


def as_bf16(mask):
    return jnp.where(mask, 1.0, 0.0).astype(jnp.bfloat16)


def log2(n):
    return n.bit_length() - 1


def flip(me, off, n):
    out = jnp.int32(0)
    bit = 1
    while bit < n:
        one = jnp.int32(bit)
        out = out + one * lax.rem(lax.div(me, one) + lax.div(off, one), jnp.int32(2))
        bit *= 2
    return out


def fold_map(shape, long_axis, group, cap):
    long, tiled = iota(shape, long_axis), iota(shape, 1 - long_axis)
    fold = long >> log2(group * cap)
    source = (long & (group * cap - 1)) >> log2(cap)
    slot = long & (cap - 1)
    return as_bf16(tiled == source * TILE + fold * cap + slot)


def dot(a, b):
    return jnp.dot(a, b, preferred_element_type=jnp.float32)


def drain(view, sem):
    pltpu.make_async_copy(view, view, sem).wait()


def attend(q, k, v, ck, cv, frames, out):
    cache_len = ck.shape[0]
    scale = 1.0 / math.sqrt(HEAD_DIM)
    usable = (iota((1, cache_len), 1) // FRAME_TOK) < frames
    contract = (((1,), (1,)), ((), ()))
    for head in range(q.shape[1] // HEAD_DIM):
        cols = slice(head * HEAD_DIM, (head + 1) * HEAD_DIM)
        query = q[:, cols]
        old = lax.dot_general(query, ck[:, cols], contract, preferred_element_type=jnp.float32)
        new = lax.dot_general(query, k[:, cols], contract, preferred_element_type=jnp.float32)
        old = jnp.where(usable, old * scale, -1e30)
        new = new * scale
        top = jnp.maximum(
            jnp.max(old, axis=1, keepdims=True), jnp.max(new, axis=1, keepdims=True)
        )
        old = jnp.exp(old - top)
        new = jnp.exp(new - top)
        total = jnp.sum(old, axis=1, keepdims=True) + jnp.sum(new, axis=1, keepdims=True)
        old = (old / total).astype(jnp.bfloat16)
        new = (new / total).astype(jnp.bfloat16)
        out[:, cols] = (dot(old, cv[:, cols]) + dot(new, v[:, cols])).astype(jnp.bfloat16)


def kernel(
    dp_n, ep_n, passes, cap, back_folds,
    frames, ids_hbm, logits_hbm, hidden_hbm,
    q_hbm, k_hbm, v_hbm, ck_hbm, cv_hbm, w1_hbm, w2_hbm,
    mixed, attended,
    ids, logits, hidden, w1, w2, q, k, v, ck, cv,
    disp, rows, xs, hid, ys, back_out, back_in,
    load_sem, disp_send, disp_recv, relay_send, relay_recv,
    hid_send, hid_recv, back_send, back_recv, own_sem,
):
    d, me = lax.axis_index("dp"), lax.axis_index("ep")
    tokens = hidden.shape[0]
    folds = TILE // cap
    fold_cols = disp.shape[2]
    back_cols = back_in.shape[2]
    group = min(ep_n, 16)
    group_rows = group * cap
    total = dp_n * ep_n

    barrier = pltpu.get_barrier_semaphore()

    def greet(i, carry):
        pl.semaphore_signal(
            barrier, inc=1, device_id={"dp": d, "ep": flip(me, i, ep_n)}, device_id_type=MESH
        )
        return carry

    lax.fori_loop(1, ep_n, greet, 0)
    for i in range(1, dp_n):
        pl.semaphore_signal(
            barrier,
            inc=1,
            device_id={"dp": lax.rem(d + i, jnp.int32(dp_n)), "ep": me},
            device_id_type=MESH,
        )

    loads = [
        pltpu.make_async_copy(src, dst, load_sem.at[i])
        for i, (src, dst) in enumerate(
            [
                (ids_hbm, ids), (logits_hbm, logits), (hidden_hbm, hidden),
                (w1_hbm, w1), (w2_hbm, w2),
                (q_hbm, q), (k_hbm, k), (v_hbm, v), (ck_hbm, ck), (cv_hbm, cv),
            ]
        )
    ]
    for load in loads:
        load.start()
    for load in loads[:3]:
        load.wait()

    experts = iota((ep_n, tokens), 0)
    named = [experts == ids[c : c + 1, :] for c in range(2)]
    count = as_bf16(named[0] | named[1])
    earlier = as_bf16(iota((tokens, tokens), 0) < iota((tokens, tokens), 1))
    before = dot(count, earlier)
    eye = iota((tokens, tokens), 0) == iota((tokens, tokens), 1)
    place, place_row, chosen = [], [], []
    for c in range(2):
        slot = jnp.sum(jnp.where(named[c], before, 0.0), axis=0, keepdims=True).astype(jnp.int32)
        turn = slot >> log2(cap)
        place_row.append((turn * ep_n + ids[c : c + 1, :]) * TILE + (slot & (cap - 1)))
        place.append(jnp.sum(jnp.where(eye, place_row[c], 0), axis=1, keepdims=True))
        chosen.append(jnp.sum(jnp.where(named[c], logits[...], 0.0), axis=0, keepdims=True))
    top = jnp.maximum(chosen[0], chosen[1])
    powers = [jnp.exp(x - top) for x in chosen]
    gates = [
        jnp.sum(jnp.where(eye, p / (powers[0] + powers[1]), 0.0), axis=1, keepdims=True)
        for p in powers
    ]

    row_at = iota((passes * ep_n * TILE, tokens), 0)
    pickers = [
        as_bf16((row_at - f * cap == place_row[0]) | (row_at - f * cap == place_row[1]))
        for f in range(folds)
    ]
    step = min(fold_cols, 256)
    for at in range(0, fold_cols, step):
        acc = dot(pickers[0], hidden[:, at : at + step])
        for f in range(1, folds):
            acc += dot(pickers[f], hidden[:, f * fold_cols + at : f * fold_cols + at + step])
        disp[:, :, at : at + step] = acc.astype(jnp.bfloat16).reshape(passes * ep_n, TILE, step)

    pl.semaphore_wait(barrier, ep_n + dp_n - 2)

    for turn in range(passes):

        def dispatch(off, carry):
            target = flip(me, off, ep_n)
            pltpu.make_async_remote_copy(
                src_ref=disp.at[turn * ep_n + target],
                dst_ref=rows.at[turn * total + d * ep_n + me],
                send_sem=disp_send,
                recv_sem=disp_recv.at[turn * ep_n + me],
                device_id={"dp": d, "ep": target},
                device_id_type=MESH,
            ).start()
            return carry

        lax.fori_loop(1, ep_n, dispatch, 0)
        pltpu.make_async_copy(
            disp.at[turn * ep_n + me],
            rows.at[turn * total + d * ep_n + me],
            disp_recv.at[turn * ep_n + me],
        ).start()

    def relay(turn, first, last):
        def one(off, carry):
            source = flip(me, off, ep_n)
            chunk = rows.at[turn * total + d * ep_n + source]
            drain(chunk, disp_recv.at[turn * ep_n + source])
            for j in range(1, dp_n):
                pltpu.make_async_remote_copy(
                    src_ref=chunk,
                    dst_ref=chunk,
                    send_sem=relay_send,
                    recv_sem=relay_recv.at[turn * dp_n + d],
                    device_id={"dp": lax.rem(d + j, jnp.int32(dp_n)), "ep": me},
                    device_id_type=MESH,
                ).start()
            return carry

        lax.fori_loop(first, last, one, 0)

    unfold = fold_map((folds * group_rows, group * TILE), 0, group, cap)
    refold = fold_map((group * TILE, back_folds * group_rows), 1, group, cap)

    def first(turn, j):
        plane = lax.rem(d + j, jnp.int32(dp_n))
        if j > 0:
            drain(rows.at[pl.ds(turn * total + plane * ep_n, ep_n)], relay_recv.at[turn * dp_n + plane])
        for g in range(ep_n // group):
            tiles = rows[pl.ds(turn * total + plane * ep_n + g * group, group)].reshape(group * TILE, fold_cols)
            flat = dot(unfold, tiles).astype(jnp.bfloat16)
            for f in range(folds):
                xs[f, g * group_rows : (g + 1) * group_rows, :] = flat[
                    f * group_rows : (f + 1) * group_rows
                ]
        acc = dot(xs[0], w1[:fold_cols, :])
        for f in range(1, folds):
            acc += dot(xs[f], w1[f * fold_cols : (f + 1) * fold_cols, :])
        hid[(turn * dp_n + plane) * dp_n + d] = jax.nn.gelu(acc, approximate=True).astype(jnp.bfloat16)
        for i in range(1, dp_n):
            pltpu.make_async_remote_copy(
                src_ref=hid.at[(turn * dp_n + plane) * dp_n + d],
                dst_ref=hid.at[(turn * dp_n + plane) * dp_n + d],
                send_sem=hid_send,
                recv_sem=hid_recv.at[(turn * dp_n + plane) * dp_n + d],
                device_id={"dp": lax.rem(d + i, jnp.int32(dp_n)), "ep": me},
                device_id_type=MESH,
            ).start()

    units = hid.shape[2]

    def second(turn, j):
        plane = lax.rem(d + j, jnp.int32(dp_n))
        for i in range(1, dp_n):
            part = (turn * dp_n + plane) * dp_n + lax.rem(d + i, jnp.int32(dp_n))
            drain(hid.at[part], hid_recv.at[part])
        for f in range(back_folds):
            cols = slice(f * back_cols, (f + 1) * back_cols)
            acc = dot(hid[(turn * dp_n + plane) * dp_n], w2[:units, cols])
            for i in range(1, dp_n):
                acc += dot(hid[(turn * dp_n + plane) * dp_n + i], w2[i * units : (i + 1) * units, cols])
            ys[f] = acc.astype(jnp.bfloat16)
        for g in range(ep_n // group):
            flat = jnp.concatenate(
                [ys[f, g * group_rows : (g + 1) * group_rows, :] for f in range(back_folds)], axis=0
            )
            tiles = dot(refold, flat).astype(jnp.bfloat16)
            back_out[pl.ds(turn * total + plane * ep_n + g * group, group)] = tiles.reshape(group, TILE, back_cols)

        def give_back(off, carry):
            target = flip(me, off, ep_n)
            pltpu.make_async_remote_copy(
                src_ref=back_out.at[turn * total + plane * ep_n + target],
                dst_ref=back_in.at[turn * total + d * ep_n + me],
                send_sem=back_send,
                recv_sem=back_recv,
                device_id={"dp": plane, "ep": target},
                device_id_type=MESH,
            ).start()
            return carry

        lax.fori_loop(1 if j == 0 else 0, ep_n, give_back, 0)
        if j == 0:
            pltpu.make_async_copy(
                back_out.at[turn * total + d * ep_n + me], back_in.at[turn * total + d * ep_n + me], own_sem
            ).start()

    planes = range(dp_n)
    relay(0, 0, ep_n)
    loads[3].wait()
    first(0, 0)
    if passes > 1:
        relay(1, 0, ep_n // 2)
    for j in planes[1:]:
        first(0, j)
    if passes > 1:
        relay(1, ep_n // 2, ep_n)
        first(1, 0)
    loads[4].wait()
    second(0, 0)
    if passes > 1:
        for j in planes[1:]:
            first(1, j)
    for j in planes[1:]:
        second(0, j)
    if passes > 1:
        for j in planes:
            second(1, j)

    for load in loads[5:]:
        load.wait()
    attend(q, k, v, ck, cv, frames[0], attended)

    col_at = iota((tokens, passes * ep_n * TILE), 1)
    picks = jnp.concatenate(
        [
            jnp.where(col_at - f * cap == place[c], 1.0, 0.0)
            for f in range(back_folds)
            for c in range(2)
        ],
        axis=0,
    ).astype(jnp.bfloat16)

    drain(back_in.at[pl.ds(0, passes * (total - 1))], back_recv)
    drain(back_in.at[pl.ds(0, passes)], own_sem)
    for h in range(dp_n):
        starts = [turn * total + h * ep_n for turn in range(passes)]
        tiles = jnp.concatenate(
            [back_in[at : at + ep_n].reshape(ep_n * TILE, back_cols) for at in starts], axis=0
        )
        picked = dot(picks, tiles)
        for f in range(back_folds):
            at = 2 * f * tokens
            cols = slice((h * back_folds + f) * back_cols, (h * back_folds + f + 1) * back_cols)
            mixed[:, cols] = (
                gates[0] * picked[at : at + tokens] + gates[1] * picked[at + tokens : at + 2 * tokens]
            ).astype(jnp.bfloat16)

    drain(disp.at[pl.ds(0, passes * (ep_n - 1))], disp_send)
    if dp_n > 1:
        drain(rows.at[pl.ds(0, passes * (dp_n - 1) * ep_n)], relay_send)
        drain(hid.at[pl.ds(0, passes * dp_n * (dp_n - 1))], hid_send)
    drain(back_out.at[pl.ds(0, passes * (total - 1))], back_send)


def shards(dp_n, ep_n, *args):
    (hidden_in, expert_ids, route_logits, first_weight, second_weight,
     queries, span_keys, span_values, cache_keys, cache_values, valid_frames) = args
    tokens, width = hidden_in.shape
    cap = max(2, 8 * tokens // (3 * ep_n))
    passes = 2 if cap % 4 == 0 else 1
    cap //= passes
    _, _, units = first_weight.shape
    _, all_units, cols = second_weight.shape
    folds = TILE // cap
    back_folds = min(folds, cols // 128)
    slots = ep_n * cap
    bf16 = jnp.bfloat16
    vmem, hbm = pl.BlockSpec(memory_space=pltpu.VMEM), pl.BlockSpec(memory_space=pltpu.HBM)
    dma = pltpu.SemaphoreType.DMA
    total = dp_n * ep_n
    streamed = (
        expert_ids.T, route_logits.T, hidden_in,
        queries, span_keys, span_values, cache_keys[0], cache_values[0],
        first_weight[0], second_weight[0],
    )
    return pl.pallas_call(
        functools.partial(kernel, dp_n, ep_n, passes, cap, back_folds),
        out_shape=(
            jax.ShapeDtypeStruct((tokens, width), bf16),
            jax.ShapeDtypeStruct(queries.shape, bf16),
        ),
        in_specs=[pl.BlockSpec(memory_space=pltpu.SMEM)] + [hbm] * len(streamed),
        out_specs=(vmem, vmem),
        scratch_shapes=[
            pltpu.VMEM((2, tokens), jnp.int32),
            pltpu.VMEM((ep_n, tokens), jnp.float32),
            pltpu.VMEM((tokens, width), bf16),
            pltpu.VMEM((width, units), bf16),
            pltpu.VMEM((all_units, cols), bf16),
            pltpu.VMEM(queries.shape, bf16),
            pltpu.VMEM(span_keys.shape, bf16),
            pltpu.VMEM(span_values.shape, bf16),
            pltpu.VMEM(cache_keys.shape[1:], bf16),
            pltpu.VMEM(cache_values.shape[1:], bf16),
            pltpu.VMEM((passes * ep_n, TILE, width // folds), bf16),
            pltpu.VMEM((passes * total, TILE, width // folds), bf16),
            pltpu.VMEM((folds, slots, width // folds), bf16),
            pltpu.VMEM((passes * dp_n * dp_n, slots, units), bf16),
            pltpu.VMEM((back_folds, slots, cols // back_folds), bf16),
            pltpu.VMEM((passes * total, TILE, cols // back_folds), bf16),
            pltpu.VMEM((passes * total, TILE, cols // back_folds), bf16),
            dma((len(streamed),)),
            dma(()),
            dma((passes * ep_n,)),
            dma(()),
            dma((passes * dp_n,)),
            dma(()),
            dma((passes * dp_n * dp_n,)),
            dma(()),
            dma(()),
            dma(()),
        ],
        compiler_params=pltpu.CompilerParams(
            collective_id=0, has_side_effects=True, vmem_limit_bytes=40 * 1024 * 1024
        ),
    )(
        valid_frames,
        *[pltpu.with_memory_space_constraint(x, pltpu.HBM) for x in streamed],
    )


def solution(mesh):
    tokens = P(("dp", "ep"), None)
    weights = P("ep", None, "dp")
    cache = P(("dp", "ep"), None, None)
    return jax.shard_map(
        functools.partial(shards, mesh.shape["dp"], mesh.shape["ep"]),
        mesh=mesh,
        in_specs=(
            tokens, tokens, tokens, weights, weights, tokens, tokens, tokens, cache, cache,
            P(("dp", "ep")),
        ),
        out_specs=(tokens, tokens),
        check_vma=False,
    )
```
